8 devices in a mesh: dp: 1 (over z), cy: 2 (over y), cx: 4 (over x, core).
Axes of the slice: x: 2, y: 2, z: 1, core: 2. Of those that a mesh axis runs over, the one named last changes fastest.
Arguments:
- q: bfloat16 [1024, 64, 128], P(('dp', 'cy', 'cx'))
- k: bfloat16 [1024, 8, 128], P(('dp', 'cy', 'cx'))
- v: bfloat16 [1024, 8, 128], P(('dp', 'cy', 'cx'))
Outputs:
- output: bfloat16 [1024, 64, 128], P(('dp', 'cy', 'cx'))
All inputs are finite; a program needn't handle non-finite values.
Results may differ from the reference program's by a relative error of at most 0.00331398.
Values are sent between devices in bfloat16 or wider.
A program may use at most 1 GiB of HBM per device.

```python
import jax
import jax.numpy as jnp
from jax import lax

SEQ = 1024
NDEV = 8
HEADS = 64
KV_HEADS = 8
HEAD_DIM = 128

SPAN = SEQ // (2 * NDEV)
NEG = -1.0e30


def positions():
    i = jnp.arange(SEQ)
    blk = i // (2 * SPAN)
    j = i % (2 * SPAN)
    return jnp.where(j < SPAN, blk * SPAN + j, (2 * NDEV - 1 - blk) * SPAN + j - SPAN)


def setup_inputs(seed: int = 0, part: int = 0) -> dict:
    key = jax.random.fold_in(jax.random.key(seed), part)
    kq, kk, kv, ko = jax.random.split(key, 4)
    q = jax.random.normal(kq, (SEQ, HEADS, HEAD_DIM), jnp.float32)
    k = jax.random.normal(kk, (SEQ, KV_HEADS, HEAD_DIM), jnp.float32)
    off = jax.random.normal(ko, (2 * NDEV, 1, KV_HEADS, HEAD_DIM), jnp.float32)
    v = 0.5 * jax.random.normal(kv, (2 * NDEV, SPAN, KV_HEADS, HEAD_DIM), jnp.float32) + off
    v = v.reshape(SEQ, KV_HEADS, HEAD_DIM)
    return {'q': q.astype(jnp.bfloat16), 'k': k.astype(jnp.bfloat16), 'v': v.astype(jnp.bfloat16)}


def reference(q, k, v):
    rep = HEADS // KV_HEADS
    scale = HEAD_DIM ** -0.5
    pos = positions().reshape(2 * NDEV, SPAN)
    qc = q.reshape(2 * NDEV, SPAN, KV_HEADS, rep, HEAD_DIM)
    kc = k.reshape(2 * NDEV, SPAN, KV_HEADS, HEAD_DIM)
    vc = v.reshape(2 * NDEV, SPAN, KV_HEADS, HEAD_DIM)

    def one_query_span(xs):
        qb, pq = xs
        qf = qb.astype(jnp.float32)

        def step(carry, ys):
            m, l, acc = carry
            kb, vb, pk = ys
            s = jnp.einsum('qgrd,kgd->grqk', qf, kb.astype(jnp.float32)) * scale
            mask = pk[None, :] <= pq[:, None]
            s = jnp.where(mask, s, NEG)
            mn = jnp.maximum(m, jnp.max(s, axis=-1))
            p = jnp.where(mask, jnp.exp(s - mn[..., None]), 0.0)
            alpha = jnp.exp(m - mn)
            l = alpha * l + jnp.sum(p, axis=-1)
            pv = jnp.einsum('grqk,kgd->grqd', p.astype(jnp.bfloat16).astype(jnp.float32), vb.astype(jnp.float32))
            acc = alpha[..., None] * acc + pv
            return (mn, l, acc), None

        init = (jnp.full((KV_HEADS, rep, SPAN), NEG, jnp.float32),
                jnp.zeros((KV_HEADS, rep, SPAN), jnp.float32),
                jnp.zeros((KV_HEADS, rep, SPAN, HEAD_DIM), jnp.float32))
        (m, l, acc), _ = lax.scan(step, init, (kc, vc, pos))
        o = (acc / l[..., None]).astype(jnp.bfloat16)
        return o.transpose(2, 0, 1, 3).reshape(SPAN, HEADS, HEAD_DIM)

    out = lax.map(one_query_span, (qc, pos))
    return out.reshape(SEQ, HEADS, HEAD_DIM)
```

```python
import functools

import jax
import jax.numpy as jnp
from jax import lax
from jax.experimental import pallas as pl
from jax.experimental.pallas import tpu as pltpu
from jax.sharding import PartitionSpec as P

NEG = -1.0e30
LOG2E = 1.4426950408889634
MESH = pl.DeviceIdType.MESH

SIB, X, Y = 1, 2, 4
LEAD = 4


def attend(qs, keys, vals, biases, c):
    nt = (((1,), (1,)), ((), ()))
    ss = []
    for k, b in zip(keys, biases):
        s = lax.dot_general(qs, k, nt, preferred_element_type=jnp.float32) * c
        ss.append(s if b is None else s + b)
    m = jnp.max(ss[0], axis=-1, keepdims=True)
    for s in ss[1:]:
        m = jnp.maximum(m, jnp.max(s, axis=-1, keepdims=True))
    return ss, m


def weigh(ss, m, vals):
    l = None
    acc = None
    for s, v in zip(ss, vals):
        p = jnp.exp2(s - m)
        pl_ = jnp.sum(p, axis=-1, keepdims=True)
        pv = jnp.dot(p.astype(jnp.bfloat16), v, preferred_element_type=jnp.float32)
        l = pl_ if l is None else l + pl_
        acc = pv if acc is None else acc + pv
    return l, acc


def main_kernel(ncx, scale, q_hbm, k_hbm, v_hbm, o_ref,
                q_s, kv_s, kin, f32s, bias_s, m_s, l_s, acc_s,
                q_sem, in_sem, ss, rs):
    nk, rows = q_s.shape[0], q_s.shape[1]
    c_rows = rows // 2
    rep = q_s.shape[2]
    hd = q_s.shape[3]
    half = c_rows * rep
    icy, icx = lax.axis_index('cy'), lax.axis_index('cx')
    dp = lax.axis_index('dp')
    me = icy * ncx + icx
    c = scale * LOG2E

    def dev(mask):
        t = me ^ mask
        return (dp, t // ncx, t % ncx)

    bar = pltpu.get_barrier_semaphore()
    for mask in (SIB, X, Y):
        pl.semaphore_signal(bar, inc=1, device_id=dev(mask), device_id_type=MESH)

    kcp = pltpu.make_async_copy(k_hbm, kin.at[0], in_sem.at[0])
    vcp = pltpu.make_async_copy(v_hbm, kin.at[1], in_sem.at[1])
    kcp.start()
    vcp.start()

    def qcopy(g):
        return pltpu.make_async_copy(q_hbm.at[:, g], q_s.at[g], q_sem.at[g])

    for g in range(nk):
        qcopy(g).start()

    def rcopy(kind, g, src, dst, mask):
        return pltpu.make_async_remote_copy(
            src_ref=src, dst_ref=dst, send_sem=ss.at[kind, g], recv_sem=rs.at[kind, g],
            device_id=dev(mask), device_id_type=MESH)

    def own(g, kind, mask):
        return rcopy(kind, g, kv_s.at[g, :, :, 0], kv_s.at[g, :, :, mask], mask)

    def own_sib(g):
        return own(g, 0, SIB)

    def own_x(g):
        return own(g, 1, X)

    def own_y(g):
        return own(g, 2, Y)

    def fwd_v(g):
        return rcopy(3, g, kv_s.at[g, 1, :, X], kv_s.at[g, 1, :, X ^ Y], Y)

    def fwd_k(g):
        return rcopy(4, g, kv_s.at[g, 0, :, Y], kv_s.at[g, 0, :, X ^ Y], X)

    def sib_x(g):
        return rcopy(5, g, kv_s.at[g, :, :, X], kv_s.at[g, :, :, X ^ SIB], SIB)

    def sib_y(g):
        return rcopy(6, g, kv_s.at[g, :, :, Y], kv_s.at[g, :, :, Y ^ SIB], SIB)

    def sib_d(g):
        return rcopy(7, g, kv_s.at[g, :, :, X ^ Y], kv_s.at[g, :, :, X ^ Y ^ SIB], SIB)

    shape = (half, 4 * c_rows)
    qi = lax.broadcasted_iota(jnp.int32, shape, 0) // rep
    col = lax.broadcasted_iota(jnp.int32, shape, 1)
    slot = col // c_rows
    kk = col % c_rows
    diag = (slot == 0) & (kk <= qi)
    e = slot ^ me
    bias_s[0] = jnp.where(diag | (e < me), 0.0, NEG)
    bias_s[1] = jnp.where(diag | (e > me), 0.0, NEG)

    kcp.wait()
    vcp.wait()
    for i in range(2):
        f32s[i] = kin[i].astype(jnp.float32).reshape(rows * nk, hd)
    for g in range(nk):
        for i in range(2):
            x = f32s[i, pl.ds(g, rows, stride=nk), :].astype(jnp.bfloat16)
            kv_s[g, i, 0, 0] = x[:c_rows]
            kv_s[g, i, 1, 0] = x[c_rows:]

    pl.semaphore_wait(bar, 3)

    for g in range(nk):
        if g < LEAD:
            own_x(g).start()
            own_y(g).start()
        own_sib(g).start()

    def keys(g, i, fs, far):
        return kv_s[g, i, fs, pl.ds(4 * far, 4)].reshape(4 * c_rows, hd)

    def qrows(g, part):
        return q_s[g, pl.ds(part * c_rows, c_rows)].reshape(half, hd)

    def save(g, part, m, l, acc):
        sl = pl.ds(part * half, half)
        m_s[g, sl, :] = jnp.broadcast_to(m, (half, hd))
        l_s[g, sl, :] = jnp.broadcast_to(l, (half, hd))
        acc_s[g, sl, :] = acc

    def finish(g, part, l, acc):
        o = (acc * (1.0 / l)).astype(jnp.bfloat16)
        o_ref[g, pl.ds(part * c_rows, c_rows)] = o.reshape(c_rows, rep, hd)

    def near(g):
        kf, ks = keys(g, 0, 0, 0), keys(g, 0, 1, 0)
        vf, vs = keys(g, 1, 0, 0), keys(g, 1, 1, 0)
        s, m = attend(qrows(g, 0), [kf], [vf], [bias_s[0]], c)
        l, acc = weigh(s, m, [vf])
        save(g, 0, m, l, acc)
        s, m = attend(qrows(g, 1), [kf, ks], [vf, vs], [None, bias_s[1]], c)
        l, acc = weigh(s, m, [vf, vs])
        save(g, 1, m, l, acc)

    def fold(g, part, kk_, vv):
        sl = pl.ds(part * half, half)
        m0, l0, acc0 = m_s[g, sl, 0:1], l_s[g, sl, 0:1], acc_s[g, sl, :]
        s, m = attend(qrows(g, part), kk_, vv, [None] * len(kk_), c)
        m = jnp.maximum(m, m0)
        l, acc = weigh(s, m, vv)
        al = jnp.exp2(m0 - m)
        finish(g, part, l0 * al + l, acc0 * al + acc)

    def far(g):
        @pl.when(icy == 0)
        def _():
            sl = pl.ds(0, half)
            finish(g, 0, l_s[g, sl, 0:1], acc_s[g, sl, :])
            fold(g, 1, [keys(g, 0, 0, 1), keys(g, 0, 1, 1)], [keys(g, 1, 0, 1), keys(g, 1, 1, 1)])

        @pl.when(icy != 0)
        def _():
            for part in range(2):
                fold(g, part, [keys(g, 0, 0, 1)], [keys(g, 1, 0, 1)])

    def take_diag(g):
        fwd_v(g).wait_recv()
        fwd_k(g).wait_recv()
        sib_d(g).start()

    def step(g, _):
        @pl.when(g < nk)
        def _():
            own_x(g).wait_recv()
            fwd_v(g).start()
            sib_x(g).start()
            own_y(g).wait_recv()
            fwd_k(g).start()
            sib_y(g).start()

            @pl.when(g + LEAD < nk)
            def _():
                own_x(g + LEAD).start()
                own_y(g + LEAD).start()

            qcopy(g).wait()
            own_sib(g).wait_recv()
            sib_x(g).wait_recv()
            near(g)

        @pl.when((g >= LEAD - 1) & (g - LEAD + 1 < nk))
        def _():
            take_diag(g - LEAD + 1)

        @pl.when(g >= LEAD)
        def _():
            h = g - LEAD
            sib_y(h).wait_recv()
            sib_d(h).wait_recv()
            far(h)
        return 0

    lax.fori_loop(0, nk + LEAD, step, 0)

    def drain(g, _):
        for f in (own_sib, own_x, own_y, fwd_v, fwd_k, sib_x, sib_y, sib_d):
            f(g).wait_send()
        return 0

    lax.fori_loop(0, nk, drain, 0)


def store_kernel(o_ref, out, sem):
    cps = [pltpu.make_async_copy(o_ref.at[g], out.at[:, g], sem.at[g]) for g in range(o_ref.shape[0])]
    for cp in cps:
        cp.start()
    for cp in cps:
        cp.wait()


def solution(mesh):
    ncx = mesh.shape['cx']
    spec = P(('dp', 'cy', 'cx'))
    bf16, f32 = jnp.bfloat16, jnp.float32

    def local(q, k, v):
        t, nh, hd = q.shape
        nk = k.shape[1]
        rep = nh // nk
        n = mesh.shape['cy'] * ncx
        c = t // 2
        scale = hd ** -0.5
        q4 = q.reshape(t, nk, rep, hd)
        hbm = pl.BlockSpec(memory_space=pltpu.HBM)
        vmem = pl.BlockSpec(memory_space=pltpu.VMEM)
        o = pl.pallas_call(
            functools.partial(main_kernel, ncx, scale),
            out_shape=pltpu.VMEM((nk, t, rep, hd), bf16),
            in_specs=[hbm, hbm, hbm],
            out_specs=vmem,
            scratch_shapes=[
                pltpu.VMEM((nk, t, rep, hd), bf16),
                pltpu.VMEM((nk, 2, 2, n, c, hd), bf16),
                pltpu.VMEM((2, t, nk, hd), bf16),
                pltpu.VMEM((2, t * nk, hd), f32),
                pltpu.VMEM((2, c * rep, 4 * c), f32),
                pltpu.VMEM((nk, t * rep, hd), f32),
                pltpu.VMEM((nk, t * rep, hd), f32),
                pltpu.VMEM((nk, t * rep, hd), f32),
                pltpu.SemaphoreType.DMA((nk,)),
                pltpu.SemaphoreType.DMA((2,)),
                pltpu.SemaphoreType.DMA((8, nk)),
                pltpu.SemaphoreType.DMA((8, nk)),
            ],
            compiler_params=pltpu.CompilerParams(
                collective_id=0, has_side_effects=True, vmem_limit_bytes=48 * 2**20),
        )(*(pltpu.with_memory_space_constraint(x, pltpu.HBM) for x in (q4, k, v)))
        o = pltpu.with_memory_space_constraint(o, pltpu.VMEM)
        out = pl.pallas_call(
            store_kernel,
            out_shape=jax.ShapeDtypeStruct((t, nk, rep, hd), bf16),
            in_specs=[vmem],
            out_specs=hbm,
            scratch_shapes=[pltpu.SemaphoreType.DMA((nk,))],
            compiler_params=pltpu.CompilerParams(vmem_limit_bytes=2**20),
        )(o)
        return out.reshape(t, nh, hd)

    return jax.shard_map(local, mesh=mesh, in_specs=(spec, spec, spec), out_specs=spec, check_vma=False)
```

```python
import functools

import jax
import jax.numpy as jnp
from jax import lax
from jax.experimental import pallas as pl
from jax.experimental.pallas import tpu as pltpu
from jax.sharding import PartitionSpec as P

NEG = -1.0e30
LOG2E = 1.4426950408889634
MESH = pl.DeviceIdType.MESH
NT = (((1,), (1,)), ((), ()))
LANES = 128

SIB, X, Y = 1, 2, 4
LEAD = 4


def lane_blocks(s):
    return [s[:, i:i + LANES] for i in range(0, s.shape[1], LANES)]


def tree(f, xs):
    xs = list(xs)
    while len(xs) > 1:
        xs = [f(*xs[i:i + 2]) if i + 1 < len(xs) else xs[i] for i in range(0, len(xs), 2)]
    return xs[0]


def scores(q, k):
    return lax.dot_general(q, k, NT, preferred_element_type=jnp.float32)


def row_max(ss):
    return jnp.max(tree(jnp.maximum, [b for s in ss for b in lane_blocks(s)]), axis=-1, keepdims=True)


def weigh(ss, vals, m, c):
    ls, acc = [], None
    for s, v in zip(ss, vals):
        ps = [jnp.exp2(b * c - m) for b in lane_blocks(s)]
        ls += ps
        p = jnp.concatenate([b.astype(jnp.bfloat16) for b in ps], axis=1)
        pv = jnp.dot(p, v, preferred_element_type=jnp.float32)
        acc = pv if acc is None else acc + pv
    return tree(jnp.add, ls), acc


def normed(l, acc):
    return (acc * (1.0 / jnp.sum(l, axis=-1, keepdims=True))).astype(jnp.bfloat16)


def fold(q, kk, vv, m0, l0, acc0, c):
    ss = [scores(q, k) for k in kk]
    m = jnp.maximum(m0, row_max(ss) * c)
    l, acc = weigh(ss, vv, m, c)
    al = jnp.exp2(m0 - m)
    return normed(l0 * al + l, acc0 * al + acc)


def far_half(icy, q, kv, m, l, acc, put, c, half):
    @pl.when(icy == 0)
    def _():
        put(0, normed(l(0), acc(0)))
        put(1, fold(q(1), [kv(0, 0), kv(0, 1)], [kv(1, 0), kv(1, 1)], m(1), l(1), acc(1), c))

    @pl.when(icy != 0)
    def _():
        for part in range(2):
            put(part, fold(q(part), [kv(0, 0)], [kv(1, 0)], m(part), l(part), acc(part), c))


def main_kernel(ncx, scale, q_hbm, k_hbm, v_hbm,
                o_ref, qz, kvz, mz, lz, accz,
                q_s, kv_s, kin, f32s, bias_s, m_s, l_s, acc_s,
                q_sem, in_sem, ss, rs):
    nk, rows, rep, hd = q_s.shape
    c_rows = rows // 2
    half = c_rows * rep
    icy, icx = lax.axis_index('cy'), lax.axis_index('cx')
    dp = lax.axis_index('dp')
    me = icy * ncx + icx
    c = scale * LOG2E

    def dev(mask):
        t = me ^ mask
        return (dp, t // ncx, t % ncx)

    bar = pltpu.get_barrier_semaphore()
    for mask in (SIB, X, Y):
        pl.semaphore_signal(bar, inc=1, device_id=dev(mask), device_id_type=MESH)

    kcp = pltpu.make_async_copy(k_hbm, kin.at[0], in_sem.at[0])
    vcp = pltpu.make_async_copy(v_hbm, kin.at[1], in_sem.at[1])
    kcp.start()
    vcp.start()

    def qcopy(g):
        return pltpu.make_async_copy(q_hbm.at[:, g], q_s.at[g], q_sem.at[g])

    for g in range(nk):
        qcopy(g).start()

    def rcopy(kind, g, src, dst, mask):
        return pltpu.make_async_remote_copy(
            src_ref=src, dst_ref=dst, send_sem=ss.at[kind, g], recv_sem=rs.at[kind, g],
            device_id=dev(mask), device_id_type=MESH)

    def own(g, kind, mask):
        return rcopy(kind, g, kv_s.at[g, :, :, 0], kv_s.at[g, :, :, mask], mask)

    def own_sib(g):
        return own(g, 0, SIB)

    def own_x(g):
        return own(g, 1, X)

    def own_y(g):
        return own(g, 2, Y)

    def fwd_v(g):
        return rcopy(3, g, kv_s.at[g, 1, :, X], kv_s.at[g, 1, :, X ^ Y], Y)

    def fwd_k(g):
        return rcopy(4, g, kv_s.at[g, 0, :, Y], kv_s.at[g, 0, :, X ^ Y], X)

    def sib_x(g):
        return rcopy(5, g, kv_s.at[g, :, :, X], kv_s.at[g, :, :, X ^ SIB], SIB)

    def sib_y(g):
        return rcopy(6, g, kv_s.at[g, :, :, Y], kv_s.at[g, :, :, Y ^ SIB], SIB)

    def sib_d(g):
        return rcopy(7, g, kv_s.at[g, :, :, X ^ Y], kv_s.at[g, :, :, X ^ Y ^ SIB], SIB)

    kcp.wait()
    vcp.wait()
    for i in range(2):
        f32s[i] = kin[i].astype(jnp.float32).reshape(rows * nk, hd)

    def head_major(g):
        for i in range(2):
            x = f32s[i, pl.ds(g, rows, stride=nk), :].astype(jnp.bfloat16)
            kv_s[g, i, 0, 0] = x[:c_rows]
            kv_s[g, i, 1, 0] = x[c_rows:]

    head_major(0)
    head_major(1)
    pl.semaphore_wait(bar, 3)
    for g in range(nk):
        if g < LEAD:
            own_x(g).start()
            own_y(g).start()
        own_sib(g).start()
        if g + 2 < nk:
            head_major(g + 2)

    shape = (half, 4 * c_rows)
    qi = lax.broadcasted_iota(jnp.int32, shape, 0) // rep
    col = lax.broadcasted_iota(jnp.int32, shape, 1)
    slot = col // c_rows
    diag = (slot == 0) & (col % c_rows <= qi)
    e = slot ^ me
    bias_s[0] = jnp.where(diag | (e < me), 0.0, NEG)
    bias_s[1] = jnp.where(diag | (e > me), 0.0, NEG)

    def keys(g, i, fs, far):
        return kv_s[g, i, fs, pl.ds(4 * far, 4)].reshape(4 * c_rows, hd)

    def q_rows(g, part):
        return q_s[g, pl.ds(part * c_rows, c_rows)].reshape(half, hd)

    def part_rows(part):
        return pl.ds(part * half, half)

    def near(g, m_ref, l_ref, acc_ref):
        kf, ks = keys(g, 0, 0, 0), keys(g, 0, 1, 0)
        vf, vs = keys(g, 1, 0, 0), keys(g, 1, 1, 0)
        q = q_s[g].reshape(2 * half, hd)
        sf = scores(q, kf)
        s_a = [sf[:half] + bias_s[0]]
        s_b = [sf[half:], scores(q[half:], ks) + bias_s[1]]
        for part, sp, vv in ((0, s_a, [vf]), (1, s_b, [vf, vs])):
            m = jnp.broadcast_to(row_max(sp) * c, (half, hd))
            l, acc = weigh(sp, vv, m, c)
            m_ref[part_rows(part)] = m
            l_ref[part_rows(part)] = l
            acc_ref[part_rows(part)] = acc

    def far(g):
        def put(part, o):
            o_ref[g, pl.ds(part * c_rows, c_rows)] = o.reshape(c_rows, rep, hd)

        far_half(icy, functools.partial(q_rows, g), lambda i, fs: keys(g, i, fs, 1),
                 lambda p: m_s[g, part_rows(p)], lambda p: l_s[g, part_rows(p)],
                 lambda p: acc_s[g, part_rows(p)], put, c, half)

    def take_own(g):
        own_x(g).wait_recv()
        fwd_v(g).start()
        sib_x(g).start()
        own_y(g).wait_recv()
        fwd_k(g).start()
        sib_y(g).start()

    def take_diag(g):
        fwd_v(g).wait_recv()
        fwd_k(g).wait_recv()
        sib_d(g).start()

    def near_step(g):
        qcopy(g).wait()
        own_sib(g).wait_recv()
        sib_x(g).wait_recv()
        near(g, m_s.at[g], l_s.at[g], acc_s.at[g])

    def far_step(g):
        sib_y(g).wait_recv()
        sib_d(g).wait_recv()
        far(g)

    last = nk - 1

    def early(g, _):
        take_own(g)

        @pl.when(g + LEAD < nk)
        def _():
            own_x(g + LEAD).start()
            own_y(g + LEAD).start()

        @pl.when(g > 0)
        def _():
            near_step(g - 1)
        return 0

    lax.fori_loop(0, LEAD, early, 0)

    def middle(g, _):
        take_own(g)
        take_diag(g - LEAD)
        near_step(g - 1)

        @pl.when(g > LEAD)
        def _():
            far_step(g - LEAD - 1)
        return 0

    lax.fori_loop(LEAD, nk, middle, 0)

    take_diag(nk - LEAD)
    qcopy(last).wait()
    own_sib(last).wait_recv()
    sib_x(last).wait_recv()
    near(last, mz, lz, accz)
    qz[...] = q_s[last].reshape(2 * half, hd)
    far_step(last - LEAD)

    def late(g, _):
        take_diag(g - LEAD)
        far_step(g - LEAD - 1)
        return 0

    lax.fori_loop(nk + 1, nk + LEAD, late, 0)

    def drain(g, _):
        for f in (own_sib, own_x, own_y, fwd_v, fwd_k, sib_x, sib_y):
            f(g).wait_send()
        return 0

    lax.fori_loop(0, nk, drain, 0)
    sib_y(last).wait_recv()
    for g in range(nk):
        sib_d(g).wait_send()
    sib_d(last).wait_recv()
    for i in range(2):
        for fs in range(2):
            kvz[i, fs] = keys(last, i, fs, 1)


def last_kernel(rows, o_ref, qz, kvz, mz, lz, accz, out, oz, sem):
    nk, _, rep, hd = o_ref.shape
    c_rows = rows // 2
    half = c_rows * rep
    cps = [pltpu.make_async_copy(o_ref.at[g], out.at[:, g], sem.at[g]) for g in range(nk - 1)]
    for cp in cps:
        cp.start()

    def part_rows(part):
        return pl.ds(part * half, half)

    def put(part, o):
        oz[pl.ds(part * c_rows, c_rows)] = o.reshape(c_rows, rep, hd)

    far_half(lax.axis_index('cy'), lambda p: qz[part_rows(p)], lambda i, fs: kvz[i, fs],
             lambda p: mz[part_rows(p)], lambda p: lz[part_rows(p)], lambda p: accz[part_rows(p)],
             put, hd ** -0.5 * LOG2E, half)
    cp = pltpu.make_async_copy(oz, out.at[:, nk - 1], sem.at[nk - 1])
    cp.start()
    for cp_ in cps:
        cp_.wait()
    cp.wait()


def solution(mesh):
    ncx = mesh.shape['cx']
    spec = P(('dp', 'cy', 'cx'))
    bf16, f32 = jnp.bfloat16, jnp.float32

    def local(q, k, v):
        t, nh, hd = q.shape
        nk = k.shape[1]
        rep = nh // nk
        n = mesh.shape['cy'] * ncx
        c = t // 2
        scale = hd ** -0.5
        q4 = q.reshape(t, nk, rep, hd)
        hbm = pl.BlockSpec(memory_space=pltpu.HBM)
        vmem = pl.BlockSpec(memory_space=pltpu.VMEM)
        outs = pl.pallas_call(
            functools.partial(main_kernel, ncx, scale),
            out_shape=(
                pltpu.VMEM((nk, t, rep, hd), bf16),
                pltpu.VMEM((t * rep, hd), bf16),
                pltpu.VMEM((2, 2, n * c // 2, hd), bf16),
                pltpu.VMEM((t * rep, hd), f32),
                pltpu.VMEM((t * rep, hd), f32),
                pltpu.VMEM((t * rep, hd), f32),
            ),
            in_specs=[hbm] * 3,
            out_specs=(vmem,) * 6,
            scratch_shapes=[
                pltpu.VMEM((nk, t, rep, hd), bf16),
                pltpu.VMEM((nk, 2, 2, n, c, hd), bf16),
                pltpu.VMEM((2, t, nk, hd), bf16),
                pltpu.VMEM((2, t * nk, hd), f32),
                pltpu.VMEM((2, c * rep, 4 * c), f32),
                pltpu.VMEM((nk - 1, t * rep, hd), f32),
                pltpu.VMEM((nk - 1, t * rep, hd), f32),
                pltpu.VMEM((nk - 1, t * rep, hd), f32),
                pltpu.SemaphoreType.DMA((nk,)),
                pltpu.SemaphoreType.DMA((2,)),
                pltpu.SemaphoreType.DMA((8, nk)),
                pltpu.SemaphoreType.DMA((8, nk)),
            ],
            compiler_params=pltpu.CompilerParams(
                collective_id=0, has_side_effects=True, vmem_limit_bytes=40 * 2**20),
        )(*(pltpu.with_memory_space_constraint(x, pltpu.HBM) for x in (q4, k, v)))
        outs = [pltpu.with_memory_space_constraint(x, pltpu.VMEM) for x in outs]
        out = pl.pallas_call(
            functools.partial(last_kernel, t),
            out_shape=jax.ShapeDtypeStruct((t, nk, rep, hd), bf16),
            in_specs=[vmem] * 6,
            out_specs=hbm,
            scratch_shapes=[pltpu.VMEM((t, rep, hd), bf16), pltpu.SemaphoreType.DMA((nk,))],
            compiler_params=pltpu.CompilerParams(vmem_limit_bytes=16 * 2**20),
        )(*outs)
        return out.reshape(t, nh, hd)

    return jax.shard_map(local, mesh=mesh, in_specs=(spec, spec, spec), out_specs=spec, check_vma=False)
```

```python
import functools

import jax
import jax.numpy as jnp
from jax import lax
from jax.experimental import pallas as pl
from jax.experimental.pallas import tpu as pltpu
from jax.sharding import PartitionSpec as P

NEG = -1.0e30
LOG2E = 1.4426950408889634
MESH = pl.DeviceIdType.MESH
NT = (((1,), (1,)), ((), ()))
LANES = 128

SIB, X, Y = 1, 2, 4
LEAD = 4


def lane_blocks(s):
    return [s[:, i:i + LANES] for i in range(0, s.shape[1], LANES)]


def tree(f, xs):
    xs = list(xs)
    while len(xs) > 1:
        xs = [f(*xs[i:i + 2]) if i + 1 < len(xs) else xs[i] for i in range(0, len(xs), 2)]
    return xs[0]


def scores(q, k):
    return lax.dot_general(q, k, NT, preferred_element_type=jnp.float32)


def row_max(ss):
    return jnp.max(tree(jnp.maximum, [b for s in ss for b in lane_blocks(s)]), axis=-1, keepdims=True)


def weigh(ss, vals, m, c):
    ls, acc = [], None
    for s, v in zip(ss, vals):
        ps = [jnp.exp2(b * c - m) for b in lane_blocks(s)]
        ls += ps
        p = jnp.concatenate([b.astype(jnp.bfloat16) for b in ps], axis=1)
        pv = jnp.dot(p, v, preferred_element_type=jnp.float32)
        acc = pv if acc is None else acc + pv
    return tree(jnp.add, ls), acc


def normed(l, acc):
    return (acc * (1.0 / jnp.sum(l, axis=-1, keepdims=True))).astype(jnp.bfloat16)


def fold(q, kk, vv, m0, l0, acc0, c):
    ss = [scores(q, k) for k in kk]
    m = jnp.maximum(m0, row_max(ss) * c)
    l, acc = weigh(ss, vv, m, c)
    al = jnp.exp2(m0 - m)
    return normed(l0 * al + l, acc0 * al + acc)


def far_half(icy, q, kv, m, l, acc, put, c, half):
    @pl.when(icy == 0)
    def _():
        put(0, normed(l(0), acc(0)))
        put(1, fold(q(1), [kv(0, 0), kv(0, 1)], [kv(1, 0), kv(1, 1)], m(1), l(1), acc(1), c))

    @pl.when(icy != 0)
    def _():
        for part in range(2):
            put(part, fold(q(part), [kv(0, 0)], [kv(1, 0)], m(part), l(part), acc(part), c))


def main_kernel(ncx, scale, q_hbm, k_hbm, v_hbm,
                o_ref, qz, kvz, mz, lz, accz,
                q_s, kv_s, kin, f32s, bias_s, m_s, l_s, acc_s,
                in_sem, ss, rs):
    nk, rows, rep, hd = q_s.shape
    c_rows = rows // 2
    half = c_rows * rep
    icy, icx = lax.axis_index('cy'), lax.axis_index('cx')
    dp = lax.axis_index('dp')
    me = icy * ncx + icx
    c = scale * LOG2E

    def dev(mask):
        t = me ^ mask
        return (dp, t // ncx, t % ncx)

    bar = pltpu.get_barrier_semaphore()
    for mask in (SIB, X, Y):
        pl.semaphore_signal(bar, inc=1, device_id=dev(mask), device_id_type=MESH)

    kcp = pltpu.make_async_copy(k_hbm, kin.at[0], in_sem.at[0])
    vcp = pltpu.make_async_copy(v_hbm, kin.at[1], in_sem.at[1])
    kcp.start()
    vcp.start()

    def rcopy(kind, arrival, g, src, dst, mask):
        return pltpu.make_async_remote_copy(
            src_ref=src, dst_ref=dst, send_sem=ss.at[kind], recv_sem=rs.at[arrival, g],
            device_id=dev(mask), device_id_type=MESH)

    def slot(g, mask, n=1):
        return kv_s.at[g, :, :, pl.ds(mask, n)]

    def own_sib(g):
        return rcopy(0, 1, g, slot(g, 0), slot(g, SIB), SIB)

    def own_x(g):
        return rcopy(1, 0, g, slot(g, 0), slot(g, X), X)

    def own_y(g):
        return rcopy(2, 0, g, slot(g, 0), slot(g, Y), Y)

    def fwd_v(g):
        return rcopy(3, 2, g, kv_s.at[g, 1, :, X], kv_s.at[g, 1, :, X ^ Y], Y)

    def fwd_k(g):
        return rcopy(4, 2, g, kv_s.at[g, 0, :, Y], kv_s.at[g, 0, :, X ^ Y], X)

    def sib_x(g):
        return rcopy(5, 1, g, slot(g, X), slot(g, X ^ SIB), SIB)

    def sib_y(g):
        return rcopy(6, 3, g, slot(g, Y), slot(g, Y ^ SIB), SIB)

    def sib_d(g):
        return rcopy(7, 3, g, slot(g, X ^ Y), slot(g, X ^ Y ^ SIB), SIB)

    def arrived(arrival, g, n):
        rcopy(0, arrival, g, slot(g, 0, n), slot(g, 0, n), SIB).wait_recv()

    kcp.wait()
    vcp.wait()
    for g in range(nk):
        pltpu.make_async_copy(q_hbm.at[:, g], q_s.at[g], in_sem.at[2]).start()
    for i in range(2):
        f32s[i] = kin[i].astype(jnp.float32).reshape(rows * nk, hd)

    def head_major(g):
        for i in range(2):
            x = f32s[i, pl.ds(g, rows, stride=nk), :].astype(jnp.bfloat16)
            kv_s[g, i, 0, 0] = x[:c_rows]
            kv_s[g, i, 1, 0] = x[c_rows:]

    head_major(0)
    head_major(1)
    pl.semaphore_wait(bar, 3)
    for g in range(nk):
        if g < LEAD:
            own_x(g).start()
            own_y(g).start()
        if g < 2:
            own_sib(g).start()
        if g + 2 < nk:
            head_major(g + 2)

    shape = (half, 4 * c_rows)
    qi = lax.broadcasted_iota(jnp.int32, shape, 0) // rep
    col = lax.broadcasted_iota(jnp.int32, shape, 1)
    at = col // c_rows
    diag = (at == 0) & (col % c_rows <= qi)
    e = at ^ me
    bias_s[0] = jnp.where(diag | (e < me), 0.0, NEG)
    bias_s[1] = jnp.where(diag | (e > me), 0.0, NEG)

    def keys(g, i, fs, far):
        return kv_s[g, i, fs, pl.ds(4 * far, 4)].reshape(4 * c_rows, hd)

    def q_rows(g, part):
        return q_s[g, pl.ds(part * c_rows, c_rows)].reshape(half, hd)

    def part_rows(part):
        return pl.ds(part * half, half)

    def near(g, m_ref, l_ref, acc_ref):
        kf, ks = keys(g, 0, 0, 0), keys(g, 0, 1, 0)
        vf, vs = keys(g, 1, 0, 0), keys(g, 1, 1, 0)
        q = q_s[g].reshape(2 * half, hd)
        sf = scores(q, kf)
        s_a = [sf[:half] + bias_s[0]]
        s_b = [sf[half:], scores(q[half:], ks) + bias_s[1]]
        for part, sp, vv in ((0, s_a, [vf]), (1, s_b, [vf, vs])):
            m = jnp.broadcast_to(row_max(sp) * c, (half, hd))
            l, acc = weigh(sp, vv, m, c)
            m_ref[part_rows(part)] = m
            l_ref[part_rows(part)] = l
            acc_ref[part_rows(part)] = acc

    def far(g):
        def put(part, o):
            o_ref[g, pl.ds(part * c_rows, c_rows)] = o.reshape(c_rows, rep, hd)

        far_half(icy, functools.partial(q_rows, g), lambda i, fs: keys(g, i, fs, 1),
                 lambda p: m_s[g, part_rows(p)], lambda p: l_s[g, part_rows(p)],
                 lambda p: acc_s[g, part_rows(p)], put, c, half)

    def take_own(g):
        arrived(0, g, 2)
        fwd_v(g).start()
        fwd_k(g).start()
        sib_x(g).start()
        sib_y(g).start()

    def take_diag(g):
        arrived(2, g, 1)
        sib_d(g).start()

    def near_step(g):
        arrived(1, g, 2)
        near(g, m_s.at[g], l_s.at[g], acc_s.at[g])

    def far_step(g):
        arrived(3, g, 2)
        far(g)

    last = nk - 1

    def early(g, _):
        take_own(g)
        own_x(g + LEAD).start()
        own_y(g + LEAD).start()
        own_sib(g + 2).start()

        @pl.when(g == 1)
        def _():
            pltpu.make_async_copy(o_ref, q_s, in_sem.at[2]).wait()

        @pl.when(g > 0)
        def _():
            near_step(g - 1)
        return 0

    lax.fori_loop(0, LEAD - 1, early, 0)

    def middle(g, _):
        take_own(g)

        @pl.when(g + LEAD < nk)
        def _():
            own_x(g + LEAD).start()
            own_y(g + LEAD).start()

        @pl.when(g + 2 < nk)
        def _():
            own_sib(g + 2).start()
        near_step(g - 1)
        take_diag(g - LEAD + 1)

        @pl.when(g >= LEAD)
        def _():
            far_step(g - LEAD)
        return 0

    lax.fori_loop(LEAD - 1, nk, middle, 0)

    arrived(1, last, 2)
    near(last, mz, lz, accz)
    qz[...] = q_s[last].reshape(2 * half, hd)
    take_diag(nk - LEAD + 1)
    far_step(nk - LEAD)
    take_diag(nk - LEAD + 2)
    take_diag(nk - LEAD + 3)

    def late(g, _):
        far_step(g)
        return 0

    lax.fori_loop(nk - LEAD + 1, last, late, 0)
    whole = kv_s.at[:, :, :, 0]
    for kind in range(8):
        ref = kv_s.at[:, 0, :, 0] if kind in (3, 4) else whole
        pltpu.make_async_remote_copy(
            src_ref=ref, dst_ref=ref, send_sem=ss.at[kind], recv_sem=rs.at[0, 0],
            device_id=dev(SIB), device_id_type=MESH).wait_send()
    arrived(3, last, 2)
    for i in range(2):
        for fs in range(2):
            kvz[i, fs] = keys(last, i, fs, 1)


def last_kernel(rows, o_ref, qz, kvz, mz, lz, accz, out, oz, sem):
    nk, _, rep, hd = o_ref.shape
    c_rows = rows // 2
    half = c_rows * rep
    cps = [pltpu.make_async_copy(o_ref.at[g], out.at[:, g], sem.at[g]) for g in range(nk - 1)]
    for cp in cps:
        cp.start()

    def part_rows(part):
        return pl.ds(part * half, half)

    def put(part, o):
        oz[pl.ds(part * c_rows, c_rows)] = o.reshape(c_rows, rep, hd)

    far_half(lax.axis_index('cy'), lambda p: qz[part_rows(p)], lambda i, fs: kvz[i, fs],
             lambda p: mz[part_rows(p)], lambda p: lz[part_rows(p)], lambda p: accz[part_rows(p)],
             put, hd ** -0.5 * LOG2E, half)
    cp = pltpu.make_async_copy(oz, out.at[:, nk - 1], sem.at[nk - 1])
    cp.start()
    for cp_ in cps:
        cp_.wait()
    cp.wait()


def solution(mesh):
    ncx = mesh.shape['cx']
    spec = P(('dp', 'cy', 'cx'))
    bf16, f32 = jnp.bfloat16, jnp.float32

    def local(q, k, v):
        t, nh, hd = q.shape
        nk = k.shape[1]
        rep = nh // nk
        n = mesh.shape['cy'] * ncx
        c = t // 2
        scale = hd ** -0.5
        q4 = q.reshape(t, nk, rep, hd)
        hbm = pl.BlockSpec(memory_space=pltpu.HBM)
        vmem = pl.BlockSpec(memory_space=pltpu.VMEM)
        outs = pl.pallas_call(
            functools.partial(main_kernel, ncx, scale),
            out_shape=(
                pltpu.VMEM((nk, t, rep, hd), bf16),
                pltpu.VMEM((t * rep, hd), bf16),
                pltpu.VMEM((2, 2, n * c // 2, hd), bf16),
                pltpu.VMEM((t * rep, hd), f32),
                pltpu.VMEM((t * rep, hd), f32),
                pltpu.VMEM((t * rep, hd), f32),
            ),
            in_specs=[hbm] * 3,
            out_specs=(vmem,) * 6,
            scratch_shapes=[
                pltpu.VMEM((nk, t, rep, hd), bf16),
                pltpu.VMEM((nk, 2, 2, n, c, hd), bf16),
                pltpu.VMEM((2, t, nk, hd), bf16),
                pltpu.VMEM((2, t * nk, hd), f32),
                pltpu.VMEM((2, c * rep, 4 * c), f32),
                pltpu.VMEM((nk - 1, t * rep, hd), f32),
                pltpu.VMEM((nk - 1, t * rep, hd), f32),
                pltpu.VMEM((nk - 1, t * rep, hd), f32),
                pltpu.SemaphoreType.DMA((3,)),
                pltpu.SemaphoreType.DMA((8,)),
                pltpu.SemaphoreType.DMA((4, nk)),
            ],
            compiler_params=pltpu.CompilerParams(
                collective_id=0, has_side_effects=True, vmem_limit_bytes=40 * 2**20),
        )(*(pltpu.with_memory_space_constraint(x, pltpu.HBM) for x in (q4, k, v)))
        outs = [pltpu.with_memory_space_constraint(x, pltpu.VMEM) for x in outs]
        out = pl.pallas_call(
            functools.partial(last_kernel, t),
            out_shape=jax.ShapeDtypeStruct((t, nk, rep, hd), bf16),
            in_specs=[vmem] * 6,
            out_specs=hbm,
            scratch_shapes=[pltpu.VMEM((t, rep, hd), bf16), pltpu.SemaphoreType.DMA((nk,))],
            compiler_params=pltpu.CompilerParams(vmem_limit_bytes=16 * 2**20),
        )(*outs)
        return out.reshape(t, nh, hd)

    return jax.shard_map(local, mesh=mesh, in_specs=(spec, spec, spec), out_specs=spec, check_vma=False)
```

```python
import functools

import jax
import jax.numpy as jnp
from jax import lax
from jax.experimental import pallas as pl
from jax.experimental.pallas import tpu as pltpu
from jax.sharding import PartitionSpec as P

NEG = -1.0e30
LOG2E = 1.4426950408889634
MESH = pl.DeviceIdType.MESH
NT = (((1,), (1,)), ((), ()))
LANES = 128

SIB, X, Y = 1, 2, 4
LOADS = 4
LEAD = 6


def lane_blocks(s):
    return [s[:, i:i + LANES] for i in range(0, s.shape[1], LANES)]


def tree(f, xs):
    xs = list(xs)
    while len(xs) > 1:
        xs = [f(*xs[i:i + 2]) if i + 1 < len(xs) else xs[i] for i in range(0, len(xs), 2)]
    return xs[0]


def scores(q, k):
    return lax.dot_general(q, k, NT, preferred_element_type=jnp.float32)


def row_max(ss):
    return jnp.max(tree(jnp.maximum, [b for s in ss for b in lane_blocks(s)]), axis=-1, keepdims=True)


def weigh(ss, vals, m, c):
    ls, acc = [], None
    for s, v in zip(ss, vals):
        ps = [jnp.exp2(b * c - m) for b in lane_blocks(s)]
        ls += ps
        p = jnp.concatenate([b.astype(jnp.bfloat16) for b in ps], axis=1)
        pv = jnp.dot(p, v, preferred_element_type=jnp.float32)
        acc = pv if acc is None else acc + pv
    return tree(jnp.add, ls), acc


def normed(l, acc):
    return (acc * (1.0 / jnp.sum(l, axis=-1, keepdims=True))).astype(jnp.bfloat16)


def fold(q, kk, vv, m0, l0, acc0, c):
    ss = [scores(q, k) for k in kk]
    m = jnp.maximum(m0, row_max(ss) * c)
    l, acc = weigh(ss, vv, m, c)
    al = jnp.exp2(m0 - m)
    return normed(l0 * al + l, acc0 * al + acc)


def far_half(icy, q, kv, m, l, acc, put, c, half):
    @pl.when(icy == 0)
    def _():
        put(0, normed(l(0), acc(0)))
        put(1, fold(q(1), [kv(0, 0), kv(0, 1)], [kv(1, 0), kv(1, 1)], m(1), l(1), acc(1), c))

    @pl.when(icy != 0)
    def _():
        for part in range(2):
            put(part, fold(q(part), [kv(0, 0)], [kv(1, 0)], m(part), l(part), acc(part), c))


def main_kernel(ncx, scale, q_hbm, k_hbm, v_hbm,
                o_ref, qz, kvz, mz, lz, accz,
                q_s, kv_s, kin, f32s, bias_s, m_s, l_s, acc_s,
                in_sem, out_sem, rs):
    nk, rows, rep, hd = q_s.shape
    c_rows = rows // 2
    half = c_rows * rep
    icy, icx = lax.axis_index('cy'), lax.axis_index('cx')
    dp = lax.axis_index('dp')
    me = icy * ncx + icx
    c = scale * LOG2E

    def dev(mask):
        t = me ^ mask
        return (dp, t // ncx, t % ncx)

    bar = pltpu.get_barrier_semaphore()
    for mask in (SIB, X, Y):
        pl.semaphore_signal(bar, inc=1, device_id=dev(mask), device_id_type=MESH)

    part = rows // LOADS
    for i in range(LOADS):
        for j, ref in enumerate((k_hbm, v_hbm)):
            sl = pl.ds(i * part, part)
            pltpu.make_async_copy(ref.at[sl], kin.at[j, sl], in_sem.at[0]).start()

    def rcopy(arrival, g, src, dst, mask):
        return pltpu.make_async_remote_copy(
            src_ref=src, dst_ref=dst, send_sem=out_sem, recv_sem=rs.at[arrival, g],
            device_id=dev(mask), device_id_type=MESH)

    def slot(g, mask, n=1):
        return kv_s.at[g, :, :, pl.ds(mask, n)]

    def own_sib(g):
        return rcopy(1, g, slot(g, 0), slot(g, SIB), SIB)

    def own_x(g):
        return rcopy(0, g, slot(g, 0), slot(g, X), X)

    def own_y(g):
        return rcopy(0, g, slot(g, 0), slot(g, Y), Y)

    def fwd_v(g):
        return rcopy(2, g, kv_s.at[g, 1, :, X], kv_s.at[g, 1, :, X ^ Y], Y)

    def fwd_k(g):
        return rcopy(2, g, kv_s.at[g, 0, :, Y], kv_s.at[g, 0, :, X ^ Y], X)

    def sib_x(g):
        return rcopy(1, g, slot(g, X), slot(g, X ^ SIB), SIB)

    def sib_y(g):
        return rcopy(3, g, slot(g, Y), slot(g, Y ^ SIB), SIB)

    def sib_d(g):
        return rcopy(3, g, slot(g, X ^ Y), slot(g, X ^ Y ^ SIB), SIB)

    def arrived(arrival, g, n):
        rcopy(arrival, g, slot(g, 0, n), slot(g, 0, n), SIB).wait_recv()

    pltpu.make_async_copy(kin, kin, in_sem.at[0]).wait()
    for g in range(nk):
        pltpu.make_async_copy(q_hbm.at[:, g], q_s.at[g], in_sem.at[1]).start()
    for i in range(2):
        f32s[i] = kin[i].astype(jnp.float32).reshape(rows * nk, hd)

    def head_major(g):
        for i in range(2):
            x = f32s[i, pl.ds(g, rows, stride=nk), :].astype(jnp.bfloat16)
            kv_s[g, i, 0, 0] = x[:c_rows]
            kv_s[g, i, 1, 0] = x[c_rows:]

    head_major(0)
    head_major(1)
    pl.semaphore_wait(bar, 3)
    for g in range(nk):
        if g < LEAD:
            own_x(g).start()
            own_y(g).start()
        own_sib(g).start()
        if g + 2 < nk:
            head_major(g + 2)

    shape = (half, 4 * c_rows)
    qi = lax.broadcasted_iota(jnp.int32, shape, 0) // rep
    col = lax.broadcasted_iota(jnp.int32, shape, 1)
    at = col // c_rows
    diag = (at == 0) & (col % c_rows <= qi)
    e = at ^ me
    bias_s[0] = jnp.where(diag | (e < me), 0.0, NEG)
    bias_s[1] = jnp.where(diag | (e > me), 0.0, NEG)

    def keys(g, i, fs, far):
        return kv_s[g, i, fs, pl.ds(4 * far, 4)].reshape(4 * c_rows, hd)

    def q_rows(g, part):
        return q_s[g, pl.ds(part * c_rows, c_rows)].reshape(half, hd)

    def part_rows(part):
        return pl.ds(part * half, half)

    def near(g, m_ref, l_ref, acc_ref):
        kf, ks = keys(g, 0, 0, 0), keys(g, 0, 1, 0)
        vf, vs = keys(g, 1, 0, 0), keys(g, 1, 1, 0)
        q = q_s[g].reshape(2 * half, hd)
        sf = scores(q, kf)
        s_a = [sf[:half] + bias_s[0]]
        s_b = [sf[half:], scores(q[half:], ks) + bias_s[1]]
        for part, sp, vv in ((0, s_a, [vf]), (1, s_b, [vf, vs])):
            m = jnp.broadcast_to(row_max(sp) * c, (half, hd))
            l, acc = weigh(sp, vv, m, c)
            m_ref[part_rows(part)] = m
            l_ref[part_rows(part)] = l
            acc_ref[part_rows(part)] = acc

    def far(g):
        def put(part, o):
            o_ref[g, pl.ds(part * c_rows, c_rows)] = o.reshape(c_rows, rep, hd)

        far_half(icy, functools.partial(q_rows, g), lambda i, fs: keys(g, i, fs, 1),
                 lambda p: m_s[g, part_rows(p)], lambda p: l_s[g, part_rows(p)],
                 lambda p: acc_s[g, part_rows(p)], put, c, half)

    def take_own(g):
        arrived(0, g, 2)
        fwd_v(g).start()
        fwd_k(g).start()
        sib_x(g).start()
        sib_y(g).start()

    def take_diag(g):
        arrived(2, g, 1)
        sib_d(g).start()

    def near_step(g):
        arrived(1, g, 2)
        near(g, m_s.at[g], l_s.at[g], acc_s.at[g])

    def far_step(g):
        arrived(3, g, 2)
        far(g)

    last = nk - 1

    def own_next(g):
        @pl.when(g + LEAD < nk)
        def _():
            own_x(g + LEAD).start()
            own_y(g + LEAD).start()

    def early(g, _):
        take_own(g)
        own_next(g)

        @pl.when(g == 1)
        def _():
            pltpu.make_async_copy(o_ref, q_s, in_sem.at[1]).wait()

        @pl.when(g > 0)
        def _():
            near_step(g - 1)
        return 0

    lax.fori_loop(0, LEAD - 1, early, 0)

    def middle(g, _):
        take_own(g)
        own_next(g)
        near_step(g - 1)
        take_diag(g - LEAD + 1)

        @pl.when(g >= LEAD)
        def _():
            far_step(g - LEAD)
        return 0

    lax.fori_loop(LEAD - 1, nk, middle, 0)

    arrived(1, last, 2)
    near(last, mz, lz, accz)
    qz[...] = q_s[last].reshape(2 * half, hd)
    take_diag(nk - LEAD + 1)

    def late(g, _):
        @pl.when(g + 2 < nk)
        def _():
            take_diag(g + 2)
        far_step(g)
        return 0

    lax.fori_loop(nk - LEAD, last, late, 0)
    ref = kv_s.at[:, :, :, pl.ds(0, 7)]
    pltpu.make_async_remote_copy(
        src_ref=ref, dst_ref=ref, send_sem=out_sem, recv_sem=rs.at[0, 0],
        device_id=dev(SIB), device_id_type=MESH).wait_send()
    arrived(3, last, 2)
    for i in range(2):
        for fs in range(2):
            kvz[i, fs] = keys(last, i, fs, 1)


def last_kernel(rows, o_ref, qz, kvz, mz, lz, accz, out, oz, sem):
    nk, _, rep, hd = o_ref.shape
    c_rows = rows // 2
    half = c_rows * rep
    cps = [pltpu.make_async_copy(o_ref.at[g], out.at[:, g], sem.at[g]) for g in range(nk - 1)]
    for cp in cps:
        cp.start()

    def part_rows(part):
        return pl.ds(part * half, half)

    def put(part, o):
        oz[pl.ds(part * c_rows, c_rows)] = o.reshape(c_rows, rep, hd)

    far_half(lax.axis_index('cy'), lambda p: qz[part_rows(p)], lambda i, fs: kvz[i, fs],
             lambda p: mz[part_rows(p)], lambda p: lz[part_rows(p)], lambda p: accz[part_rows(p)],
             put, hd ** -0.5 * LOG2E, half)
    cp = pltpu.make_async_copy(oz, out.at[:, nk - 1], sem.at[nk - 1])
    cp.start()
    for cp_ in cps:
        cp_.wait()
    cp.wait()


def solution(mesh):
    ncx = mesh.shape['cx']
    spec = P(('dp', 'cy', 'cx'))
    bf16, f32 = jnp.bfloat16, jnp.float32

    def local(q, k, v):
        t, nh, hd = q.shape
        nk = k.shape[1]
        rep = nh // nk
        n = mesh.shape['cy'] * ncx
        c = t // 2
        scale = hd ** -0.5
        q4 = q.reshape(t, nk, rep, hd)
        hbm = pl.BlockSpec(memory_space=pltpu.HBM)
        vmem = pl.BlockSpec(memory_space=pltpu.VMEM)
        outs = pl.pallas_call(
            functools.partial(main_kernel, ncx, scale),
            out_shape=(
                pltpu.VMEM((nk, t, rep, hd), bf16),
                pltpu.VMEM((t * rep, hd), bf16),
                pltpu.VMEM((2, 2, n * c // 2, hd), bf16),
                pltpu.VMEM((t * rep, hd), f32),
                pltpu.VMEM((t * rep, hd), f32),
                pltpu.VMEM((t * rep, hd), f32),
            ),
            in_specs=[hbm] * 3,
            out_specs=(vmem,) * 6,
            scratch_shapes=[
                pltpu.VMEM((nk, t, rep, hd), bf16),
                pltpu.VMEM((nk, 2, 2, n, c, hd), bf16),
                pltpu.VMEM((2, t, nk, hd), bf16),
                pltpu.VMEM((2, t * nk, hd), f32),
                pltpu.VMEM((2, c * rep, 4 * c), f32),
                pltpu.VMEM((nk - 1, t * rep, hd), f32),
                pltpu.VMEM((nk - 1, t * rep, hd), f32),
                pltpu.VMEM((nk - 1, t * rep, hd), f32),
                pltpu.SemaphoreType.DMA((2,)),
                pltpu.SemaphoreType.DMA,
                pltpu.SemaphoreType.DMA((4, nk)),
            ],
            compiler_params=pltpu.CompilerParams(
                collective_id=0, has_side_effects=True, vmem_limit_bytes=40 * 2**20),
        )(*(pltpu.with_memory_space_constraint(x, pltpu.HBM) for x in (q4, k, v)))
        outs = [pltpu.with_memory_space_constraint(x, pltpu.VMEM) for x in outs]
        out = pl.pallas_call(
            functools.partial(last_kernel, t),
            out_shape=jax.ShapeDtypeStruct((t, nk, rep, hd), bf16),
            in_specs=[vmem] * 6,
            out_specs=hbm,
            scratch_shapes=[pltpu.VMEM((t, rep, hd), bf16), pltpu.SemaphoreType.DMA((nk,))],
            compiler_params=pltpu.CompilerParams(vmem_limit_bytes=16 * 2**20),
        )(*outs)
        return out.reshape(t, nh, hd)

    return jax.shard_map(local, mesh=mesh, in_specs=(spec, spec, spec), out_specs=spec, check_vma=False)
```

```python
import functools

import jax
import jax.numpy as jnp
from jax import lax
from jax.experimental import pallas as pl
from jax.experimental.pallas import tpu as pltpu
from jax.sharding import PartitionSpec as P

NEG = -1.0e30
LOG2E = 1.4426950408889634
MESH = pl.DeviceIdType.MESH
NT = (((1,), (1,)), ((), ()))
LANES = 128

SIB, X, Y = 1, 2, 4
LOADS = 4
LEAD = 6


def lane_blocks(s):
    return [s[:, i:i + LANES] for i in range(0, s.shape[1], LANES)]


def tree(f, xs):
    xs = list(xs)
    while len(xs) > 1:
        xs = [f(*xs[i:i + 2]) if i + 1 < len(xs) else xs[i] for i in range(0, len(xs), 2)]
    return xs[0]


def scores(q, k):
    return lax.dot_general(q, k, NT, preferred_element_type=jnp.float32)


def row_max(ss):
    return jnp.max(tree(jnp.maximum, [b for s in ss for b in lane_blocks(s)]), axis=-1, keepdims=True)


def weigh(ss, vals, m, c):
    ls, acc = [], None
    for s, v in zip(ss, vals):
        ps = [jnp.exp2(b * c - m) for b in lane_blocks(s)]
        ls += ps
        p = jnp.concatenate([b.astype(jnp.bfloat16) for b in ps], axis=1)
        pv = jnp.dot(p, v, preferred_element_type=jnp.float32)
        acc = pv if acc is None else acc + pv
    return tree(jnp.add, ls), acc


def start_state(ss, vals, c):
    m = jnp.broadcast_to(row_max(ss) * c, (ss[0].shape[0], LANES))
    return (m,) + weigh(ss, vals, m, c)


def fold(state, q, kk, vv, c):
    m0, l0, acc0 = state
    ss = [scores(q, k) for k in kk]
    m = jnp.maximum(m0, row_max(ss) * c)
    l, acc = weigh(ss, vv, m, c)
    al = jnp.exp2(m0 - m)
    return m, l0 * al + l, acc0 * al + acc


class Head:
    def __init__(self, q, kv, m, l, acc):
        self.q, self.kv, self.state = q, kv, (m, l, acc)
        self.t, self.rep, self.hd = q.shape
        self.half = self.t // 2 * self.rep

    def rows(self, part):
        n = self.t // 2
        return self.q[pl.ds(part * n, n)].reshape(self.half, self.hd)

    def both(self, i, p):
        return self.kv[i, p].reshape(2 * self.t, self.hd)

    def first(self, i, p):
        return self.kv[i, p, 0].reshape(self.t, self.hd)

    def load(self, part):
        return tuple(r[pl.ds(part * self.half, self.half)] for r in self.state)

    def save(self, part, state):
        for r, x in zip(self.state, state):
            r[pl.ds(part * self.half, self.half)] = x

    def fold(self, part, keys, c):
        return fold(self.load(part), self.rows(part), keys(0), keys(1), c)

    def normed(self, state):
        _, l, acc = state
        o = (acc * (1.0 / jnp.sum(l, axis=-1, keepdims=True))).astype(jnp.bfloat16)
        return o.reshape(self.t // 2, self.rep, self.hd)

    def far(self, cy, put, c):
        if cy == 0:
            put(1, self.normed(self.fold(1, lambda i: [self.both(i, 2), self.both(i, 3)], c)))
        else:
            for part in range(2):
                keys = lambda i: [jnp.concatenate([self.first(i, 2), self.first(i, 3)], axis=0)]
                put(part, self.normed(self.fold(part, keys, c)))


def main_kernel(ncx, scale, q_hbm, k_hbm, v_hbm,
                o_ref, q_s, kv_s, m_s, l_s, acc_s,
                kin, f32s, bias_s, in_sem, out_sem, rs):
    nk, rows, rep, hd = q_s.shape
    c_rows = rows // 2
    half = c_rows * rep
    icy, icx = lax.axis_index('cy'), lax.axis_index('cx')
    dp = lax.axis_index('dp')
    me = icy * ncx + icx
    c = scale * LOG2E

    def dev(mask):
        t = me ^ mask
        return (dp, t // ncx, t % ncx)

    bar = pltpu.get_barrier_semaphore()
    for mask in (SIB, X, Y):
        pl.semaphore_signal(bar, inc=1, device_id=dev(mask), device_id_type=MESH)

    part = rows // LOADS
    for i in range(LOADS):
        for j, ref in enumerate((k_hbm, v_hbm)):
            sl = pl.ds(i * part, part)
            pltpu.make_async_copy(ref.at[sl], kin.at[j, sl], in_sem.at[0]).start()

    def rcopy(arrival, g, src, dst, mask):
        return pltpu.make_async_remote_copy(
            src_ref=src, dst_ref=dst, send_sem=out_sem, recv_sem=rs.at[arrival, g],
            device_id=dev(mask), device_id_type=MESH)

    def slot(g, mask, i=None):
        if i is None:
            return kv_s.at[g, :, mask // 2, :, mask % 2]
        return kv_s.at[g, i, mask // 2, :, mask % 2]

    def own_sib(g):
        return rcopy(4, g, slot(g, 0), slot(g, SIB), SIB)

    def own_x(g):
        return rcopy(0, g, slot(g, 0), slot(g, X), X)

    def own_y(g):
        return rcopy(0, g, slot(g, 0), slot(g, Y), Y)

    def fwd_v(g):
        return rcopy(2, g, slot(g, X, 1), slot(g, X ^ Y, 1), Y)

    def fwd_k(g):
        return rcopy(2, g, slot(g, Y, 0), slot(g, X ^ Y, 0), X)

    def sib_x(g):
        return rcopy(1, g, slot(g, X), slot(g, X ^ SIB), SIB)

    def sib_y(g):
        return rcopy(3, g, slot(g, Y), slot(g, Y ^ SIB), SIB)

    def sib_d(g):
        return rcopy(3, g, slot(g, X ^ Y), slot(g, X ^ Y ^ SIB), SIB)

    def arrived(arrival, g, n):
        ref = kv_s.at[g, :, 0] if n == 2 else slot(g, 0)
        rcopy(arrival, g, ref, ref, SIB).wait_recv()

    pltpu.make_async_copy(kin, kin, in_sem.at[0]).wait()
    for g in range(nk):
        pltpu.make_async_copy(q_hbm.at[:, g], q_s.at[g], in_sem.at[1]).start()
    for i in range(2):
        f32s[i] = kin[i].astype(jnp.float32).reshape(rows * nk, hd)

    def head_major(g):
        for i in range(2):
            x = f32s[i, pl.ds(g, rows, stride=nk), :].astype(jnp.bfloat16)
            kv_s[g, i, 0, 0, 0] = x[:c_rows]
            kv_s[g, i, 0, 1, 0] = x[c_rows:]

    head_major(0)
    head_major(1)
    pl.semaphore_wait(bar, 3)
    for g in range(nk):
        if g < LEAD:
            own_x(g).start()
            own_y(g).start()
        own_sib(g).start()
        if g + 2 < nk:
            head_major(g + 2)

    shape = (half, 2 * c_rows)
    qi = lax.broadcasted_iota(jnp.int32, shape, 0) // rep
    col = lax.broadcasted_iota(jnp.int32, shape, 1)
    at = col // c_rows
    diag = (at == 0) & (col % c_rows <= qi)
    e = at ^ me
    bias_s[0] = jnp.where(diag | (e < me), 0.0, NEG)
    bias_s[1] = jnp.where(diag | (e > me), 0.0, NEG)

    def head(g):
        return Head(q_s.at[g], kv_s.at[g], m_s.at[g], l_s.at[g], acc_s.at[g])

    def put_o(g, part, o):
        o_ref[g, pl.ds(part * c_rows, c_rows)] = o

    def local(g):
        h = head(g)
        s = scores(h.rows(0), h.first(0, 0)) + bias_s[0]
        st = start_state([s], [h.first(1, 0)], c)
        h.save(0, st)
        s = scores(h.rows(1), h.both(0, 0))
        s = jnp.concatenate([s[:, :2 * c_rows], s[:, 2 * c_rows:] + bias_s[1]], axis=1)
        h.save(1, start_state([s], [h.both(1, 0)], c))

    def side(g):
        h = head(g)

        @pl.when(icx < ncx // 2)
        def _():
            h.save(1, h.fold(1, lambda i: [h.both(i, 1)], c))

        @pl.when(icx >= ncx // 2)
        def _():
            for part in range(2):
                h.save(part, h.fold(part, lambda i: [h.first(i, 1)], c))

    def far(g):
        h = head(g)

        @pl.when(icy == 0)
        def _():
            put_o(g, 0, h.normed(h.load(0)))
            h.far(0, functools.partial(put_o, g), c)

        @pl.when(icy != 0)
        def _():
            h.far(1, functools.partial(put_o, g), c)

    def take_own(g):
        arrived(0, g, 2)
        fwd_v(g).start()
        fwd_k(g).start()
        sib_x(g).start()
        sib_y(g).start()

    def take_diag(g):
        arrived(2, g, 1)
        sib_d(g).start()

    last = nk - 1
    pltpu.make_async_copy(o_ref, q_s, in_sem.at[1]).wait()

    def local_step(g, _):
        arrived(4, g, 1)
        local(g)
        return 0

    lax.fori_loop(0, nk, local_step, 0)

    def side_step(g):
        arrived(1, g, 1)
        side(g)

    def far_step(g):
        arrived(3, g, 2)
        far(g)

    def step(g, _):
        take_own(g)

        @pl.when(g + LEAD < nk)
        def _():
            own_x(g + LEAD).start()
            own_y(g + LEAD).start()

        @pl.when(g > 0)
        def _():
            side_step(g - 1)

        @pl.when(g >= LEAD - 1)
        def _():
            take_diag(g - LEAD + 1)

        @pl.when(g >= LEAD)
        def _():
            far_step(g - LEAD)
        return 0

    lax.fori_loop(0, nk, step, 0)
    side_step(last)
    take_diag(nk - LEAD + 1)

    def late(g, _):
        @pl.when(g + 2 < nk)
        def _():
            take_diag(g + 2)
        far_step(g)
        return 0

    lax.fori_loop(nk - LEAD, last, late, 0)
    ref = kv_s.at[pl.ds(0, 7)]
    pltpu.make_async_remote_copy(
        src_ref=ref, dst_ref=ref, send_sem=out_sem, recv_sem=rs.at[0, 0],
        device_id=dev(SIB), device_id_type=MESH).wait_send()
    arrived(3, last, 2)


def last_kernel(o_ref, q_s, kv_s, m_s, l_s, acc_s, out, oz, sem):
    nk, t, rep, hd = o_ref.shape
    last = nk - 1
    cps = [pltpu.make_async_copy(o_ref.at[g], out.at[:, g], sem.at[g]) for g in range(last)]
    for cp in cps:
        cp.start()
    h = Head(*(r.at[last] for r in (q_s, kv_s, m_s, l_s, acc_s)))

    def put(part, o):
        oz[pl.ds(part * t // 2, t // 2)] = o

    for cy in (0, 1):
        @pl.when(lax.axis_index('cy') == cy)
        def _():
            if cy == 0:
                put(0, h.normed(h.load(0)))
            h.far(cy, put, hd ** -0.5 * LOG2E)

    cps.append(pltpu.make_async_copy(oz, out.at[:, last], sem.at[last]))
    cps[-1].start()
    for cp in cps:
        cp.wait()


def solution(mesh):
    ncx = mesh.shape['cx']
    spec = P(('dp', 'cy', 'cx'))
    bf16, f32 = jnp.bfloat16, jnp.float32

    def local(q, k, v):
        t, nh, hd = q.shape
        nk = k.shape[1]
        rep = nh // nk
        n = mesh.shape['cy'] * ncx
        c = t // 2
        scale = hd ** -0.5
        q4 = q.reshape(t, nk, rep, hd)
        hbm = pl.BlockSpec(memory_space=pltpu.HBM)
        vmem = pl.BlockSpec(memory_space=pltpu.VMEM)
        outs = pl.pallas_call(
            functools.partial(main_kernel, ncx, scale),
            out_shape=(
                pltpu.VMEM((nk, t, rep, hd), bf16),
                pltpu.VMEM((nk, t, rep, hd), bf16),
                pltpu.VMEM((nk, 2, n // 2, 2, 2, c, hd), bf16),
                pltpu.VMEM((nk, t * rep, hd), f32),
                pltpu.VMEM((nk, t * rep, hd), f32),
                pltpu.VMEM((nk, t * rep, hd), f32),
            ),
            in_specs=[hbm] * 3,
            out_specs=(vmem,) * 6,
            scratch_shapes=[
                pltpu.VMEM((2, t, nk, hd), bf16),
                pltpu.VMEM((2, t * nk, hd), f32),
                pltpu.VMEM((2, c * rep, 2 * c), f32),
                pltpu.SemaphoreType.DMA((2,)),
                pltpu.SemaphoreType.DMA,
                pltpu.SemaphoreType.DMA((5, nk)),
            ],
            compiler_params=pltpu.CompilerParams(
                collective_id=0, has_side_effects=True, vmem_limit_bytes=16 * 2**20),
        )(*(pltpu.with_memory_space_constraint(x, pltpu.HBM) for x in (q4, k, v)))
        outs = [pltpu.with_memory_space_constraint(x, pltpu.VMEM) for x in outs]
        out = pl.pallas_call(
            last_kernel,
            out_shape=jax.ShapeDtypeStruct((t, nk, rep, hd), bf16),
            in_specs=[vmem] * 6,
            out_specs=hbm,
            scratch_shapes=[pltpu.VMEM((t, rep, hd), bf16), pltpu.SemaphoreType.DMA((nk,))],
            compiler_params=pltpu.CompilerParams(vmem_limit_bytes=8 * 2**20),
        )(*outs)
        return out.reshape(t, nh, hd)

    return jax.shard_map(local, mesh=mesh, in_specs=(spec, spec, spec), out_specs=spec, check_vma=False)
```
